32 devices in a mesh: seq: 8 (over z, x), head: 4 (over y, core).
Axes of the slice: x: 2, y: 2, z: 4, core: 2. Of those that a mesh axis runs over, the one named last changes fastest.
Arguments:
- x_in: bfloat16 [8192, 4096], P('seq', 'head'), may hold values from -6 to 6
- z_gate: bfloat16 [8192, 4096], P('seq', 'head'), may hold values from -6 to 6
- b_in: bfloat16 [8192, 128], P('seq', 'head'), may hold values from -2 to 2
- c_in: bfloat16 [8192, 128], P('seq', 'head'), may hold values from -2 to 2
- dt_raw: float32 [8192, 64], P('seq', 'head'), may hold values from -4 to 4
- decay_rate: float32 [64], P('head'), may hold values from 6.1035156e-05 to 0.05, as said below
- skip_gain: float32 [64], P('head'), may hold values from 0.5 to 1.5
- norm_gain: float32 [4096], P('head'), may hold values from 0.1 to 1.9
- w_out: bfloat16 [4096, 2560], P('head'), may hold values from -0.09375 to 0.09375
- doc_lengths: int32 [32], replicated, may hold values from 1 to 2048, 8192 in all
Outputs:
- mixed: bfloat16 [8192, 2560], P(('seq', 'head'))
The draws below stay inside these ranges and needn't reach their ends.
Inputs may be any that keep to these rules, and one draw needn't show every extreme that they name: `decay_rate`: every head's rate lies in the range. `doc_lengths`: they sum to 8192; the longest is exactly 2048.
All inputs are finite; a program needn't handle non-finite values.
Results may differ from the reference program's by a relative error of at most 0.018.
Values may be sent and summed in bfloat16 or wider, within the bound.
A program may use at most 128 MiB of HBM per device.

```python
import math
import jax
import jax.numpy as jnp
import numpy as np
from jax import lax

D = 2560
HEADS = 64
HEAD_DIM = 64
STATE = 128
SPAN = 256
DOCS = 32
TOKENS = 8192
DOC_MOST = 2048
N_HEAD = 4


def draw_decay_rate(key, part):
    uniform_draw = jax.random.uniform(jax.random.fold_in(key, 11), (HEADS,), jnp.float32)
    lowest = 0.5 / TOKENS
    highest = 0.05
    return jnp.exp(jnp.log(lowest) + uniform_draw * (jnp.log(highest) - jnp.log(lowest))).astype(jnp.float32)


def block_levels(stream_key, shape, cuts, low, high):
    factor_of = 1.0
    for axis_at, blocks in cuts:
        draws = jax.random.uniform(jax.random.fold_in(jax.random.fold_in(stream_key, 6), axis_at), (blocks,), jnp.float32, low / len(cuts), high / len(cuts))
        factor_of = factor_of * jnp.repeat(jnp.exp(draws), shape[axis_at] // blocks).reshape((-1,) + (1,) * (len(shape) - 1 - axis_at))
    return factor_of


def split_up(number_of, total, limit, lean):
    weights = [(1 << 20) // math.isqrt(rank ** lean) + 1 for rank in range(2, number_of + 1)]
    rest, given = total - limit - (number_of - 1), [1] * (number_of - 1)
    while rest > 0:
        movable = [i for i in range(number_of - 1) if given[i] < limit]
        mass, left = sum([weights[i] for i in movable]), rest
        for i in movable:
            extra = min(limit - given[i], max(1, left * weights[i] // mass), rest)
            given[i] = given[i] + extra
            rest = rest - extra
    return np.array([limit] + given)


def uneven_parts(rng, number_of, total, most, slope):
    if number_of == 2:
        one = jax.random.randint(rng, (), max(1, total - most), min(most, total - 1) + 1)
        return jnp.stack([one, total - one])
    sizes = jnp.asarray(split_up(number_of, total, most, slope), jnp.int32)
    twos = (number_of - 1) // 2
    giver, sink = sizes[1:1 + 2 * twos:2], sizes[2:2 + 2 * twos:2]
    margin = jnp.minimum(giver - 1, most - sink)
    shifted = jax.random.randint(jax.random.fold_in(rng, 1), (twos,), 0, 1 << 20) % (margin + 1)
    sizes = sizes.at[1:1 + 2 * twos:2].set(giver - shifted).at[2:2 + 2 * twos:2].set(sink + shifted)
    return sizes[jax.random.permutation(jax.random.fold_in(rng, 2), number_of)]


def bell_draw(key, extent, spread, limit, shards=(), kind=jnp.bfloat16):
    entries = jax.random.normal(key, extent, jnp.float32) * spread
    if len(shards) > 0:
        entries = block_levels(key, extent, shards, -0.22, 0.18) * entries
    return jnp.clip(entries, min=-limit, max=limit).astype(kind)


def setup_inputs(seed: int = 0) -> dict:
    splits = jax.random.split(jax.random.key(seed), 11)
    return {
        "x_in": bell_draw(splits[0], (TOKENS, HEADS * HEAD_DIM), 1.0, 6.0, ((0, 8), (1, 4))),
        "z_gate": bell_draw(splits[1], (TOKENS, HEADS * HEAD_DIM), 1.0, 6.0, ((0, 8), (1, 4))),
        "b_in": bell_draw(splits[2], (TOKENS, STATE), 0.3, 2.0, ((0, 8), (1, 4))),
        "c_in": bell_draw(splits[3], (TOKENS, STATE), 0.3, 2.0, ((0, 8), (1, 4))),
        "dt_raw": bell_draw(splits[4], (TOKENS, HEADS), 1.0, 4.0, ((0, 8), (1, 4)), jnp.float32),
        "decay_rate": draw_decay_rate(jax.random.fold_in(splits[10], 71), 0),
        "skip_gain": jnp.clip(0.5 + 1.0 * jax.random.uniform(splits[6], (HEADS,), jnp.float32) ** block_levels(splits[6], (HEADS,), ((0, 4),), -0.2, 0.2), 0.5, 1.5),
        "norm_gain": jnp.clip(1.0 + 0.18 * jax.random.normal(splits[7], (HEADS * HEAD_DIM,), jnp.float32), 0.1, 1.9),
        "w_out": bell_draw(splits[8], (HEADS * HEAD_DIM, D), (HEADS * HEAD_DIM) ** -0.5, 0.09375, ((0, 4),)),
        "doc_lengths": uneven_parts(splits[9], DOCS, TOKENS, DOC_MOST, 2).astype(jnp.int32),
    }


norm_eps = 1e-05

def reference(x_in, z_gate, b_in, c_in, dt_raw, decay_rate, skip_gain, norm_gain, w_out, doc_lengths):
    inner_width = HEADS * HEAD_DIM
    block_width = inner_width // N_HEAD
    positions = jnp.arange(TOKENS, dtype=jnp.int32)
    doc_ends = jnp.cumsum(doc_lengths).astype(jnp.int32)
    doc_starts = (doc_ends - doc_lengths).astype(jnp.int32)
    doc_ids = lax.optimization_barrier(jnp.sum((positions[:, None] >= doc_ends[None, :]).astype(jnp.int32), axis=1)).astype(jnp.int32)
    start_flags = jnp.any(positions[:, None] == doc_starts[None, :], axis=1).astype(jnp.int32)
    step_size = jax.nn.softplus(dt_raw)
    log_decay = -step_size * decay_rate[None, :]
    spans = TOKENS // SPAN
    inputs = x_in.reshape(spans, SPAN, HEADS, HEAD_DIM)
    gates = z_gate.reshape(spans, SPAN, inner_width)
    b_blocks = b_in.reshape(spans, SPAN, STATE)
    c_blocks = c_in.reshape(spans, SPAN, STATE)
    step_blocks = step_size.reshape(spans, SPAN, HEADS)
    decay_blocks = log_decay.reshape(spans, SPAN, HEADS)
    id_blocks = doc_ids.reshape(spans, SPAN)
    flag_blocks = start_flags.reshape(spans, SPAN)
    w_blocks = w_out.astype(jnp.float32).reshape(N_HEAD, block_width, D)
    local_pos = jnp.arange(SPAN, dtype=jnp.int32)
    causal_mask = local_pos[:, None] >= local_pos[None, :]

    def span_step(carried, pieces):
        xc, zc, bc, cc, steps_here, decay_here, ids_here, flags_here = pieces
        cumulative = jnp.cumsum(decay_here, axis=0)
        scores = jnp.dot(cc, bc.T, preferred_element_type=jnp.float32)
        same_doc = causal_mask & (ids_here[:, None] == ids_here[None, :])
        cum_heads = cumulative.T
        differ = cum_heads[:, :, None] - cum_heads[:, None, :]
        decay_table = jnp.exp(jnp.where(same_doc[None], differ, -jnp.inf))
        weights = (scores[None] * decay_table * steps_here.T[:, None, :]).astype(jnp.bfloat16)
        y_local = jnp.einsum('hij,jhp->ihp', weights.astype(jnp.float32), xc.astype(jnp.float32))
        unreset = (jnp.cumsum(flags_here) == 0).astype(jnp.float32)
        from_start = jnp.exp(cumulative) * unreset[:, None]
        y_inter = jnp.einsum('in,hpn->ihp', cc.astype(jnp.float32), carried, precision=lax.Precision.HIGHEST) * from_start[:, :, None]
        y_total = y_local + y_inter + skip_gain[None, :, None] * xc.astype(jnp.float32)
        to_end = jnp.exp(cumulative[-1][None, :] - cumulative) * (ids_here == ids_here[-1])[:, None].astype(jnp.float32)
        scaled = (xc.astype(jnp.float32) * (to_end * steps_here)[:, :, None]).astype(jnp.bfloat16)
        block_state = jnp.einsum('jhp,jn->hpn', scaled.astype(jnp.float32), bc.astype(jnp.float32))
        new_state = from_start[-1][:, None, None] * carried + block_state
        gated = y_total.reshape(SPAN, inner_width) * jax.nn.silu(zc.astype(jnp.float32))
        inverse_rms = lax.rsqrt(lax.optimization_barrier(jnp.mean(gated * gated, axis=1)) + norm_eps)
        normed = (gated * norm_gain[None, :]).astype(jnp.bfloat16)
        partials = jnp.einsum('qkc,kcd->kqd', normed.astype(jnp.float32).reshape(SPAN, N_HEAD, block_width), w_blocks)
        summed = lax.optimization_barrier(jnp.sum(partials.astype(jnp.bfloat16).astype(jnp.float32), axis=0))
        return (new_state, (summed * inverse_rms[:, None]).astype(jnp.bfloat16))
    initial = jnp.zeros((HEADS, HEAD_DIM, STATE), jnp.float32)
    _, out_rows = lax.scan(span_step, initial, (inputs, gates, b_blocks, c_blocks, step_blocks, decay_blocks, id_blocks, flag_blocks))
    return out_rows.reshape(TOKENS, D)
```

```python
import functools

import jax
import jax.numpy as jnp
from jax import lax
from jax.experimental import pallas as pl
from jax.experimental.pallas import tpu as pltpu
from jax.sharding import PartitionSpec as P

norm_eps = 1e-05
MESH = pl.DeviceIdType.MESH
F32, BF16 = jnp.float32, jnp.bfloat16


def halves(v):
    high = v.astype(BF16).astype(F32)
    return high, v - high


def kernel(
    dims,
    bc_ref,
    dt_ref,
    rate_ref,
    skip_ref,
    gain_ref,
    ends_ref,
    x_hbm,
    z_hbm,
    w_hbm,
    out_ref,
    x_v,
    z_v,
    w_v,
    bc_all,
    xf_v,
    at_v,
    g_v,
    dec_v,
    cal_v,
    y_v,
    eg_v,
    st_send,
    st_recv,
    gin_v,
    nrm_v,
    own_v,
    a_send,
    a_recv,
    b_send,
    b_recv,
    sq_send,
    sq_recv,
    loc_sem,
    bc_ssem,
    bc_rsem,
    st_ssem,
    st_rsem,
    sq_ssem,
    sq_rsem,
    a_ssem,
    a_rsem,
    b_ssem,
    b_rsem,
):
    n_seq, groups, blk, heads, reach, chunks = dims
    rows, width = x_v.shape
    part = bc_ref.shape[0] // 2
    n_state = part * groups
    head_size = width // heads
    cw = w_v.shape[1] // chunks
    hd = lax.axis_index("head")
    sq = lax.axis_index("seq")
    p1 = hd + 1 - 2 * (hd % 2)
    p2 = (hd + 2) % 4
    p3 = (p1 + 2) % 4
    rel = (hd, p1, p2, p3)

    loads = [
        pltpu.make_async_copy(src, dst, loc_sem.at[i])
        for i, (src, dst) in enumerate(
            ((x_hbm, x_v), (z_hbm, z_v), (w_hbm, w_v), (bc_ref, bc_all.at[hd]))
        )
    ]
    loads[0].start()
    loads[3].start()

    barrier = pltpu.get_barrier_semaphore()
    for k in (1, 2, 3):
        pl.semaphore_signal(
            barrier, inc=1, device_id={"seq": sq, "head": rel[k]}, device_id_type=MESH
        )
    for k in range(1, reach + 1):
        for other in ((sq + k) % n_seq, (sq + n_seq - k) % n_seq):
            pl.semaphore_signal(
                barrier, inc=1, device_id={"seq": other, "head": hd}, device_id_type=MESH
            )
    pl.semaphore_wait(barrier, 3 + 2 * reach)

    def to_head(k, src, dst, ssem, rsem):
        return pltpu.make_async_remote_copy(
            src_ref=src,
            dst_ref=dst,
            send_sem=ssem,
            recv_sem=rsem,
            device_id={"seq": sq, "head": rel[k]},
            device_id_type=MESH,
        )

    bc_copies = [
        to_head(k, bc_ref, bc_all.at[hd], bc_ssem.at[k], bc_rsem.at[k]) for k in (1, 2, 3)
    ]
    for copy in bc_copies:
        copy.start()
    loads[1].start()
    loads[2].start()

    step = jnp.log(1.0 + jnp.exp(dt_ref[...]))
    ld = -step * rate_ref[...]
    l1, rest = halves(ld)
    l2, l3 = halves(rest)
    split = jnp.concatenate([l1, l2, l3], axis=0).astype(BF16)
    ii = lax.broadcasted_iota(jnp.int32, (blk, blk), 0)
    jj = lax.broadcasted_iota(jnp.int32, (blk, blk), 1)
    upper = jnp.where(ii <= jj, 1.0, 0.0).astype(BF16)
    er = lax.broadcasted_iota(jnp.int32, (128, width), 0)
    ec = lax.broadcasted_iota(jnp.int32, (128, width), 1)
    lead = ec // head_size
    spread_f = jnp.where((er == lead) | (er == lead + heads), 1.0, 0.0).astype(BF16)
    spread_e = jnp.where(
        (er == lead + 2 * heads) | (er == lead + 3 * heads), 1.0, 0.0
    ).astype(BF16)
    pad = jnp.zeros((128 - 4 * heads, blk), F32)
    lasts = []
    for s in range(groups):
        at = slice(s * blk, (s + 1) * blk)
        c3 = jnp.dot(split[:, at], upper, preferred_element_type=F32)
        cum = c3[:heads] + c3[heads : 2 * heads] + c3[2 * heads :]
        fh, fl = halves(jnp.exp(-cum) * step[:, at])
        eh, el = halves(jnp.exp(cum))
        turned = jnp.concatenate([fh, fl, eh, el, pad], axis=0).T.astype(BF16)
        at_v[s] = turned
        lasts.append(
            jnp.dot(turned[blk - 16 :], spread_e, preferred_element_type=F32)[15:16]
        )
        if s == 0:
            loads[0].wait()
        fx = jnp.dot(turned, spread_f, preferred_element_type=F32)
        xf_v[s] = (x_v[at, :].astype(F32) * fx).astype(BF16)

    base = sq * rows
    pos = base + lax.broadcasted_iota(jnp.int32, (8, rows), 1)
    doc = jnp.zeros((8, rows), F32)
    marks = [base + s * blk - 1 for s in range(groups + 1)]
    tags = [jnp.float32(0.0)] * (groups + 1)
    for k in range(ends_ref.shape[0]):
        end = ends_ref[k]
        doc = doc + jnp.where(pos >= end, 1.0, 0.0)
        tags = [t + jnp.where(m >= end, 1.0, 0.0) for t, m in zip(tags, marks)]

    for copy in bc_copies:
        copy.wait_recv()
    loads[3].wait()
    bt = jnp.concatenate([bc_all[k, :part, :] for k in range(groups)], axis=0)
    ct = jnp.concatenate([bc_all[k, part:, :] for k in range(groups)], axis=0)

    state = jnp.zeros((n_state, width), F32)
    decay = jnp.ones((1, width), F32)
    for s in range(groups):
        at = slice(s * blk, (s + 1) * blk)
        g_v[s] = state.astype(BF16)
        dec_v[s] = jnp.broadcast_to(decay, (8, width))
        kept = jnp.where(doc[:1, at] == tags[s + 1], 1.0, 0.0)
        bm = (bt[:, at].astype(F32) * kept).astype(BF16)
        grown = jnp.dot(bm, xf_v[s], preferred_element_type=F32)
        alive = jnp.where(tags[s] == tags[s + 1], 1.0, 0.0)
        state = lasts[s] * (alive * state + grown)
        decay = decay * (lasts[s] * alive)
    st_send[:n_state, :] = state.astype(BF16)
    st_send[n_state:, :] = jnp.broadcast_to(decay, (16, width)).astype(BF16)

    def to_later(k):
        return pltpu.make_async_remote_copy(
            src_ref=st_send,
            dst_ref=st_recv.at[k - 1],
            send_sem=st_ssem.at[k - 1],
            recv_sem=st_rsem.at[k - 1],
            device_id={"seq": (sq + k) % n_seq, "head": hd},
            device_id_type=MESH,
        )

    for k in range(1, reach + 1):

        @pl.when(sq + k < n_seq)
        def _():
            to_later(k).start()

    loads[1].wait()
    for s in range(groups):
        at = slice(s * blk, (s + 1) * blk)
        c_s = ct[:, at].astype(F32).T
        scores = jnp.dot(c_s.astype(BF16), bt[:, at], preferred_element_type=F32)
        row = doc[:1, at]
        col = jnp.broadcast_to(row, (128, blk)).T[:, :1]
        seen = (ii >= jj) & (col == row)
        scores = jnp.where(seen, scores, 0.0).astype(BF16)
        cal = (c_s * jnp.where(col == tags[s], 1.0, 0.0)).astype(BF16)
        cal_v[s] = cal
        ex = jnp.dot(at_v[s], spread_e, preferred_element_type=F32)
        y = jnp.dot(scores, xf_v[s], preferred_element_type=F32)
        y = y + jnp.dot(cal, g_v[s], preferred_element_type=F32)
        zf = z_v[at, :].astype(F32)
        gate = zf / (1.0 + jnp.exp(-zf))
        y_v[s] = (ex * y + skip_ref[...] * x_v[at, :].astype(F32)) * gate
        eg_v[s] = ex * gate

    for k in range(1, reach + 1):

        @pl.when(sq >= k)
        def _():
            to_later(k).wait_recv()

        @pl.when(sq < k)
        def _():
            st_recv[k - 1] = jnp.zeros(st_recv.shape[1:], BF16)

    incoming = jnp.zeros((n_state, width), F32)
    for k in range(reach, 0, -1):
        incoming = (
            st_recv[k - 1, :n_state, :].astype(F32)
            + st_recv[k - 1, n_state : n_state + 1, :].astype(F32) * incoming
        )
    gin_v[...] = incoming

    def normed_of(q):
        carried = (gin_v[...] * dec_v[q][:1]).astype(BF16)
        u = y_v[q] + eg_v[q] * jnp.dot(cal_v[q], carried, preferred_element_type=F32)
        total = jnp.sum(u * u, axis=1, keepdims=True)
        nrm_v[...] = (u * gain_ref[...]).astype(BF16)
        return jnp.broadcast_to(total, (blk, 128)).T[:8]

    def product(c):
        return jnp.dot(nrm_v[...], w_v[:, c * cw : (c + 1) * cw], preferred_element_type=F32)

    def a_copy(t, c):
        i = t * chunks + c
        return to_head(1, a_send.at[i], a_recv.at[i], a_ssem.at[i], a_rsem.at[i])

    def b_copy(c):
        return to_head(2, b_send.at[c], b_recv.at[c], b_ssem.at[c], b_rsem.at[c])

    def sq_copy(k):
        return to_head(
            k, sq_send.at[k], sq_recv.at[k], sq_ssem.at[k], sq_rsem.at[k]
        )

    loads[2].wait()
    for t, k in ((0, 3), (None, 2), (1, 1), (None, 0)):
        sq_send[k] = normed_of(rel[k])
        if k:
            sq_copy(k).start()
        for c in range(chunks):
            cut = slice(c * cw, (c + 1) * cw)
            term = product(c)
            if t is not None:
                a_send[t * chunks + c] = term.astype(BF16)
                a_copy(t, c).start()
            elif k == 2:
                a_copy(0, c).wait_recv()
                b_send[c] = (term + a_recv[c].astype(F32)).astype(BF16)
                b_copy(c).start()
            else:
                own_v[:, cut] = term
    for k in (1, 2, 3):
        sq_copy(k).wait_recv()
    squares = sq_send[0] + sq_recv[1] + sq_recv[2] + sq_recv[3]
    squares = jnp.broadcast_to(squares[:1], (128, blk)).T[:, :1]
    inverse = lax.rsqrt(squares / (width * groups) + norm_eps)
    for c in range(chunks):
        cut = slice(c * cw, (c + 1) * cw)
        a_copy(1, c).wait_recv()
        b_copy(c).wait_recv()
        total = own_v[:, cut] + a_recv[chunks + c].astype(F32) + b_recv[c].astype(F32)
        out_ref[:, cut] = (total * inverse).astype(BF16)
    for copy in bc_copies:
        copy.wait_send()
    for k in range(1, reach + 1):

        @pl.when(sq + k < n_seq)
        def _():
            to_later(k).wait_send()

    for k in (1, 2, 3):
        sq_copy(k).wait_send()
    for c in range(chunks):
        a_copy(0, c).wait_send()
        a_copy(1, c).wait_send()
        b_copy(c).wait_send()


def on_device(
    x_in, z_gate, b_in, c_in, dt_raw, decay_rate, skip_gain, norm_gain, w_out, doc_lengths
):
    rows, width = x_in.shape
    heads = dt_raw.shape[1]
    head_size = width // heads
    groups, n_seq = lax.axis_size("head"), lax.axis_size("seq")
    blk = rows // groups
    longest = rows * n_seq // 4
    reach = min(-(-(longest - 1) // rows), n_seq - 1)
    d_model = w_out.shape[1]
    chunks = 5
    part = b_in.shape[1]
    n_state = part * groups
    bc = jnp.concatenate([b_in.T, c_in.T], axis=0)
    ends = jnp.cumsum(doc_lengths)
    skip = jnp.repeat(skip_gain, head_size)[None, :]
    cw = d_model // chunks
    vm = pl.BlockSpec(memory_space=pltpu.VMEM)
    hbm = pl.BlockSpec(memory_space=pl.ANY)
    dma = pltpu.SemaphoreType.DMA
    return pl.pallas_call(
        functools.partial(kernel, (n_seq, groups, blk, heads, reach, chunks)),
        out_shape=jax.ShapeDtypeStruct((blk, d_model), BF16),
        in_specs=[vm] * 5 + [pl.BlockSpec(memory_space=pltpu.SMEM)] + [hbm] * 3,
        out_specs=vm,
        scratch_shapes=[
            pltpu.VMEM((rows, width), BF16),
            pltpu.VMEM((rows, width), BF16),
            pltpu.VMEM(w_out.shape, BF16),
            pltpu.VMEM((groups, 2 * part, rows), BF16),
            pltpu.VMEM((groups, blk, width), BF16),
            pltpu.VMEM((groups, blk, 128), BF16),
            pltpu.VMEM((groups, n_state, width), BF16),
            pltpu.VMEM((groups, 8, width), F32),
            pltpu.VMEM((groups, blk, n_state), BF16),
            pltpu.VMEM((groups, blk, width), F32),
            pltpu.VMEM((groups, blk, width), F32),
            pltpu.VMEM((n_state + 16, width), BF16),
            pltpu.VMEM((reach, n_state + 16, width), BF16),
            pltpu.VMEM((n_state, width), F32),
            pltpu.VMEM((blk, width), BF16),
            pltpu.VMEM((blk, d_model), F32),
            pltpu.VMEM((2 * chunks, blk, cw), BF16),
            pltpu.VMEM((2 * chunks, blk, cw), BF16),
            pltpu.VMEM((chunks, blk, cw), BF16),
            pltpu.VMEM((chunks, blk, cw), BF16),
            pltpu.VMEM((4, 8, blk), F32),
            pltpu.VMEM((4, 8, blk), F32),
            dma((4,)),
            dma((4,)),
            dma((4,)),
            dma((reach,)),
            dma((reach,)),
            dma((4,)),
            dma((4,)),
            dma((2 * chunks,)),
            dma((2 * chunks,)),
            dma((chunks,)),
            dma((chunks,)),
        ],
        compiler_params=pltpu.CompilerParams(
            collective_id=0, has_side_effects=True, vmem_limit_bytes=60 * 1024 * 1024
        ),
        name="layer",
    )(bc, dt_raw.T, decay_rate[:, None], skip, norm_gain[None, :], ends, x_in, z_gate, w_out)


def solution(mesh):
    return jax.shard_map(
        on_device,
        mesh=mesh,
        in_specs=(
            P("seq", "head"),
            P("seq", "head"),
            P("seq", "head"),
            P("seq", "head"),
            P("seq", "head"),
            P("head"),
            P("head"),
            P("head"),
            P("head", None),
            P(),
        ),
        out_specs=P(("seq", "head"), None),
        check_vma=False,
    )
```

```python
import functools

import jax
import jax.numpy as jnp
from jax import lax
from jax.experimental import pallas as pl
from jax.experimental.pallas import tpu as pltpu
from jax.sharding import PartitionSpec as P

norm_eps = 1e-05
MESH = pl.DeviceIdType.MESH
F32, BF16 = jnp.float32, jnp.bfloat16


def halves(v):
    high = v.astype(BF16).astype(F32)
    return high, v - high


def kernel(
    dims,
    b_ref,
    c_ref,
    dt_ref,
    gain_ref,
    rate_ref,
    skip_ref,
    lengths_ref,
    x_hbm,
    z_hbm,
    w_hbm,
    out_ref,
    x_v,
    z_v,
    w_v,
    turn_v,
    maps_v,
    xf_v,
    at_v,
    g_v,
    dec_v,
    cal_v,
    y_v,
    eg_v,
    st_send,
    st_recv,
    dc_send,
    dc_recv,
    gin_v,
    nrm_v,
    own_v,
    a_send,
    a_recv,
    b_send,
    b_recv,
    sq_send,
    sq_recv,
    loc_sem,
    mp_ssem,
    mp_rsem,
    st_ssem,
    st_rsem,
    sq_ssem,
    sq_rsem,
    a_ssem,
    a_rsem,
    b_ssem,
    b_rsem,
):
    n_seq, groups, blk, heads, reach, chunks = dims
    rows, width = x_v.shape
    part = b_ref.shape[1]
    n_state = part * groups
    head_size = width // heads
    cw = w_v.shape[1] // chunks
    hd = lax.axis_index("head")
    sq = lax.axis_index("seq")
    p1 = hd + 1 - 2 * (hd % 2)
    p2 = (hd + 2) % 4
    p3 = (p1 + 2) % 4
    rel = (hd, p1, p2, p3)

    loads = [
        pltpu.make_async_copy(src, dst, loc_sem.at[i])
        for i, (src, dst) in enumerate(
            ((x_hbm, x_v), (z_hbm, z_v), (w_hbm, w_v))
        )
    ]
    loads[0].start()

    barrier = pltpu.get_barrier_semaphore()
    for k in (1, 2, 3):
        pl.semaphore_signal(
            barrier, inc=1, device_id={"seq": sq, "head": rel[k]}, device_id_type=MESH
        )
    for k in range(1, reach + 1):
        for other in ((sq + k) % n_seq, (sq + n_seq - k) % n_seq):
            pl.semaphore_signal(
                barrier, inc=1, device_id={"seq": other, "head": hd}, device_id_type=MESH
            )
    turn_v[:, :part] = b_ref[...].astype(F32)
    turn_v[:, part : 2 * part] = c_ref[...].astype(F32)
    turn_v[:, 2 * part : 2 * part + heads] = dt_ref[...]
    turned = turn_v[...].T
    maps_v[0, 0] = turned[:part].astype(BF16)
    maps_v[1, 0] = turned[part : 2 * part].astype(BF16)
    dt_rows = turned[2 * part : 2 * part + heads]
    pl.semaphore_wait(barrier, 3 + 2 * reach)

    def to_head(k, src, dst, ssem, rsem):
        return pltpu.make_async_remote_copy(
            src_ref=src,
            dst_ref=dst,
            send_sem=ssem,
            recv_sem=rsem,
            device_id={"seq": sq, "head": rel[k]},
            device_id_type=MESH,
        )

    def map_copy(i, k):
        source = maps_v.at[i, 2 if k == 3 else 0]
        j = 4 * i + k
        return to_head(
            1 if k == 3 else k, source, maps_v.at[i, k], mp_ssem.at[j], mp_rsem.at[j]
        )

    for i in (0, 1):
        map_copy(i, 2).start()
        map_copy(i, 1).start()
    loads[1].start()
    loads[2].start()

    step = jnp.log(1.0 + jnp.exp(dt_rows))
    which = lax.broadcasted_iota(jnp.int32, (heads, 128), 0)
    lane_head = lax.broadcasted_iota(jnp.int32, (1, width), 1) // head_size
    rate = jnp.zeros((heads, 128), F32)
    skip = jnp.zeros((1, width), F32)
    for h in range(heads):
        rate = jnp.where(which == h, rate_ref[h], rate)
        skip = jnp.where(lane_head == h, skip_ref[h], skip)
    ld = -step * rate[:, :1]
    l1, rest = halves(ld)
    l2, l3 = halves(rest)
    split = jnp.concatenate([l1, l2, l3], axis=0).astype(BF16)
    ii = lax.broadcasted_iota(jnp.int32, (blk, blk), 0)
    jj = lax.broadcasted_iota(jnp.int32, (blk, blk), 1)
    upper = jnp.where(ii <= jj, 1.0, 0.0).astype(BF16)
    er = lax.broadcasted_iota(jnp.int32, (128, width), 0)
    ec = lax.broadcasted_iota(jnp.int32, (128, width), 1)
    lead = ec // head_size
    spread_f = jnp.where((er == lead) | (er == lead + heads), 1.0, 0.0).astype(BF16)
    spread_e = jnp.where(
        (er == lead + 2 * heads) | (er == lead + 3 * heads), 1.0, 0.0
    ).astype(BF16)
    pad = jnp.zeros((128 - 4 * heads, blk), F32)
    lasts, finals = [], []
    for s in range(groups):
        at = slice(s * blk, (s + 1) * blk)
        c3 = jnp.dot(split[:, at], upper, preferred_element_type=F32)
        cum = c3[:heads] + c3[heads : 2 * heads] + c3[2 * heads :]
        fh, fl = halves(jnp.exp(-cum) * step[:, at])
        grow = jnp.exp(cum)
        finals.append(jnp.broadcast_to(grow[:, blk - 1 :], (heads, 128)))
        eh, el = halves(grow)
        turned = jnp.concatenate([fh, fl, eh, el, pad], axis=0).T.astype(BF16)
        at_v[s] = turned
        lasts.append(
            jnp.dot(turned[blk - 16 :], spread_e, preferred_element_type=F32)[15:16]
        )
        if s == 0:
            loads[0].wait()
        fx = jnp.dot(turned, spread_f, preferred_element_type=F32)
        xf_v[s] = (x_v[at, :].astype(F32) * fx).astype(BF16)

    base = sq * rows
    pos = base + lax.broadcasted_iota(jnp.int32, (8, rows), 1)
    doc = jnp.zeros((8, rows), F32)
    marks = [base + s * blk - 1 for s in range(groups + 1)]
    tags = [jnp.float32(0.0)] * (groups + 1)
    end = 0
    for k in range(lengths_ref.shape[0]):
        end = end + lengths_ref[k]
        doc = doc + jnp.where(pos >= end, 1.0, 0.0)
        tags = [t + jnp.where(m >= end, 1.0, 0.0) for t, m in zip(tags, marks)]

    map_copy(0, 2).wait_recv()
    map_copy(0, 3).start()

    def later(j, k, source, place):
        i = 3 * (k - 1) + j
        return pltpu.make_async_remote_copy(
            src_ref=source,
            dst_ref=place.at[k - 1] if j == 2 else place.at[k - 1, j],
            send_sem=st_ssem.at[i],
            recv_sem=st_rsem.at[i],
            device_id={"seq": (sq + k) % n_seq, "head": hd},
            device_id_type=MESH,
        )

    def to_later(j, k):
        if j == 2:
            return later(j, k, dc_send, dc_recv)
        return later(j, k, st_send.at[j], st_recv)

    def send_later(j):
        for k in range(1, reach + 1):

            @pl.when(sq + k < n_seq)
            def _():
                to_later(j, k).start()

    half = n_state // 2
    decay = jnp.ones((1, width), F32)
    whole = jnp.ones((heads, 128), F32)
    alives = []
    for s in range(groups):
        dec_v[s] = jnp.broadcast_to(decay, (8, width))
        alive = jnp.where(tags[s] == tags[s + 1], 1.0, 0.0)
        alives.append(alive)
        decay = decay * (lasts[s] * alive)
        whole = whole * (finals[s] * alive)
    dc_send[...] = whole.astype(BF16)
    send_later(2)
    for j in (0, 1):
        map_copy(0, 2 * j + 1).wait_recv()
        bt = jnp.concatenate([maps_v[0, 2 * j], maps_v[0, 2 * j + 1]], axis=0)
        state = jnp.zeros((half, width), F32)
        for s in range(groups):
            at = slice(s * blk, (s + 1) * blk)
            g_v[s, j * half : (j + 1) * half, :] = state.astype(BF16)
            kept = jnp.where(doc[:1, at] == tags[s + 1], 1.0, 0.0)
            bm = (bt[:, at].astype(F32) * kept).astype(BF16)
            grown = jnp.dot(bm, xf_v[s], preferred_element_type=F32)
            state = lasts[s] * (alives[s] * state + grown)
        st_send[j] = state.astype(BF16)
        send_later(j)
        if j == 0:
            map_copy(1, 2).wait_recv()
            map_copy(1, 3).start()
    map_copy(1, 1).wait_recv()
    map_copy(1, 3).wait_recv()
    bt = jnp.concatenate([maps_v[0, k] for k in range(groups)], axis=0)
    ct = jnp.concatenate([maps_v[1, k] for k in range(groups)], axis=0)

    loads[1].wait()
    for s in range(groups):
        at = slice(s * blk, (s + 1) * blk)
        c_s = ct[:, at].astype(F32).T
        scores = jnp.dot(c_s.astype(BF16), bt[:, at], preferred_element_type=F32)
        row = doc[:1, at]
        col = jnp.broadcast_to(row, (128, blk)).T[:, :1]
        seen = (ii >= jj) & (col == row)
        scores = jnp.where(seen, scores, 0.0).astype(BF16)
        cal = (c_s * jnp.where(col == tags[s], 1.0, 0.0)).astype(BF16)
        cal_v[s] = cal
        ex = jnp.dot(at_v[s], spread_e, preferred_element_type=F32)
        y = jnp.dot(scores, xf_v[s], preferred_element_type=F32)
        y = y + jnp.dot(cal, g_v[s], preferred_element_type=F32)
        zf = z_v[at, :].astype(F32)
        gate = zf / (1.0 + jnp.exp(-zf))
        y_v[s] = (ex * y + skip * x_v[at, :].astype(F32)) * gate
        eg_v[s] = ex * gate

    loads[2].wait()
    for k in range(1, reach + 1):

        @pl.when(sq >= k)
        def _():
            for j in (2, 0, 1):
                to_later(j, k).wait_recv()

        @pl.when(sq < k)
        def _():
            st_recv[k - 1] = jnp.zeros(st_recv.shape[1:], BF16)
            dc_recv[k - 1] = jnp.zeros(dc_recv.shape[1:], BF16)

    fill = jnp.zeros((128 - heads, 128), F32)
    incoming = jnp.zeros((n_state, width), F32)
    for k in range(reach, 0, -1):
        came = st_recv[k - 1].reshape(n_state, width).astype(F32)
        if k < reach:
            turned = jnp.concatenate([dc_recv[k - 1].astype(F32), fill], axis=0).T[:16]
            times = jnp.dot(turned.astype(BF16), spread_f, preferred_element_type=F32)
            came = came + times[:1] * incoming
        incoming = came
    gin_v[...] = incoming

    def normed_of(q, slot):
        carried = (gin_v[...] * dec_v[q][:1]).astype(BF16)
        u = y_v[q] + eg_v[q] * jnp.dot(cal_v[q], carried, preferred_element_type=F32)
        total = jnp.sum(u * u, axis=1, keepdims=True)
        nrm_v[slot] = (u * gain_ref[...]).astype(BF16)
        return jnp.broadcast_to(total, (blk, 128)).T[:8]

    def product(c, slot):
        return jnp.dot(
            nrm_v[slot], w_v[:, c * cw : (c + 1) * cw], preferred_element_type=F32
        )

    def a_copy(t, c):
        i = t * chunks + c
        return to_head(1, a_send.at[i], a_recv.at[i], a_ssem.at[i], a_rsem.at[i])

    def b_copy(c):
        return to_head(2, b_send.at[c], b_recv.at[c], b_ssem.at[c], b_rsem.at[c])

    def sq_copy(k):
        return to_head(
            k, sq_send.at[k], sq_recv.at[k], sq_ssem.at[k], sq_rsem.at[k]
        )

    def give(t, c, slot):
        a_send[t * chunks + c] = product(c, slot).astype(BF16)
        a_copy(t, c).start()

    def pass_on(c):
        term = product(c, 1)
        a_copy(0, c).wait_recv()
        b_send[c] = (term + a_recv[c].astype(F32)).astype(BF16)
        b_copy(c).start()

    sums3 = normed_of(p3, 0)
    give(0, 0, 0)
    sums2 = normed_of(p2, 1)
    for c in range(chunks):
        if c + 1 < chunks:
            give(0, c + 1, 0)
        pass_on(c)
    sq_send[3] = sums3
    sq_send[2] = sums2
    sq_copy(3).start()
    sq_copy(2).start()
    sq_send[1] = normed_of(p1, 0)
    sq_copy(1).start()
    for c in range(chunks):
        give(1, c, 0)
    sq_send[0] = normed_of(hd, 1)
    for c in range(chunks):
        own_v[:, c * cw : (c + 1) * cw] = product(c, 1)
    for k in (1, 2, 3):
        sq_copy(k).wait_recv()
    squares = sq_send[0] + sq_recv[1] + sq_recv[2] + sq_recv[3]
    squares = jnp.broadcast_to(squares[:1], (128, blk)).T[:, :1]
    inverse = lax.rsqrt(squares / (width * groups) + norm_eps)
    for c in range(chunks):
        cut = slice(c * cw, (c + 1) * cw)
        a_copy(1, c).wait_recv()
        b_copy(c).wait_recv()
        total = own_v[:, cut] + a_recv[chunks + c].astype(F32) + b_recv[c].astype(F32)
        out_ref[:, cut] = (total * inverse).astype(BF16)
    for i in (0, 1):
        for k in (1, 2, 3):
            map_copy(i, k).wait_send()
    for k in range(1, reach + 1):

        @pl.when(sq + k < n_seq)
        def _():
            for j in (0, 1, 2):
                to_later(j, k).wait_send()

    for k in (1, 2, 3):
        sq_copy(k).wait_send()
    for c in range(chunks):
        a_copy(0, c).wait_send()
        a_copy(1, c).wait_send()
        b_copy(c).wait_send()


def on_device(
    x_in, z_gate, b_in, c_in, dt_raw, decay_rate, skip_gain, norm_gain, w_out, doc_lengths
):
    rows, width = x_in.shape
    heads = dt_raw.shape[1]
    head_size = width // heads
    groups, n_seq = lax.axis_size("head"), lax.axis_size("seq")
    blk = rows // groups
    longest = rows * n_seq // 4
    reach = min(-(-(longest - 1) // rows), n_seq - 1)
    d_model = w_out.shape[1]
    chunks = 5
    part = b_in.shape[1]
    n_state = part * groups
    cw = d_model // chunks
    vm = pl.BlockSpec(memory_space=pltpu.VMEM)
    hbm = pl.BlockSpec(memory_space=pl.ANY)
    dma = pltpu.SemaphoreType.DMA
    return pl.pallas_call(
        functools.partial(kernel, (n_seq, groups, blk, heads, reach, chunks)),
        out_shape=jax.ShapeDtypeStruct((blk, d_model), BF16),
        in_specs=[vm] * 4 + [pl.BlockSpec(memory_space=pltpu.SMEM)] * 3 + [hbm] * 3,
        out_specs=vm,
        scratch_shapes=[
            pltpu.VMEM((rows, width), BF16),
            pltpu.VMEM((rows, width), BF16),
            pltpu.VMEM(w_out.shape, BF16),
            pltpu.VMEM((rows, 128), F32),
            pltpu.VMEM((2, groups, part, rows), BF16),
            pltpu.VMEM((groups, blk, width), BF16),
            pltpu.VMEM((groups, blk, 128), BF16),
            pltpu.VMEM((groups, n_state, width), BF16),
            pltpu.VMEM((groups, 8, width), F32),
            pltpu.VMEM((groups, blk, n_state), BF16),
            pltpu.VMEM((groups, blk, width), F32),
            pltpu.VMEM((groups, blk, width), F32),
            pltpu.VMEM((2, n_state // 2, width), BF16),
            pltpu.VMEM((reach, 2, n_state // 2, width), BF16),
            pltpu.VMEM((heads, 128), BF16),
            pltpu.VMEM((reach, heads, 128), BF16),
            pltpu.VMEM((n_state, width), F32),
            pltpu.VMEM((2, blk, width), BF16),
            pltpu.VMEM((blk, d_model), F32),
            pltpu.VMEM((2 * chunks, blk, cw), BF16),
            pltpu.VMEM((2 * chunks, blk, cw), BF16),
            pltpu.VMEM((chunks, blk, cw), BF16),
            pltpu.VMEM((chunks, blk, cw), BF16),
            pltpu.VMEM((4, 8, blk), F32),
            pltpu.VMEM((4, 8, blk), F32),
            dma((3,)),
            dma((8,)),
            dma((8,)),
            dma((3 * reach,)),
            dma((3 * reach,)),
            dma((4,)),
            dma((4,)),
            dma((2 * chunks,)),
            dma((2 * chunks,)),
            dma((chunks,)),
            dma((chunks,)),
        ],
        compiler_params=pltpu.CompilerParams(
            collective_id=0, has_side_effects=True, vmem_limit_bytes=60 * 1024 * 1024
        ),
        name="layer",
    )(
        b_in,
        c_in,
        dt_raw,
        norm_gain[None, :],
        decay_rate,
        skip_gain,
        doc_lengths,
        x_in,
        z_gate,
        w_out,
    )


def solution(mesh):
    return jax.shard_map(
        on_device,
        mesh=mesh,
        in_specs=(
            P("seq", "head"),
            P("seq", "head"),
            P("seq", "head"),
            P("seq", "head"),
            P("seq", "head"),
            P("head"),
            P("head"),
            P("head"),
            P("head", None),
            P(),
        ),
        out_specs=P(("seq", "head"), None),
        check_vma=False,
    )
```
